32 devices in a mesh: tensor: 8 (over z, y), dp: 4 (over x, core).
Axes of the slice: x: 2, y: 2, z: 4, core: 2. Of those that a mesh axis runs over, the one named last changes fastest.
Arguments:
- base_weight: bfloat16 [2, 2, 4096, 14336], P(None, None, 'tensor', 'dp'), may hold values from -0.125 to 0.125
- adapter_left: bfloat16 [2, 2, 4096, 16], P(None, None, 'tensor'), may hold values from -0.059814453 to 0.059814453
- adapter_right: bfloat16 [2, 2, 16, 14336], P(None, None, None, 'dp'), may hold values from -1.5 to 1.5
- magnitude: bfloat16 [2, 2, 14336], P(None, None, 'dp'), may hold values from 16 to 256
Outputs:
- merged_weight: bfloat16 [2, 2, 14336, 4096], P(None, None, 'tensor')
The draws below stay inside these ranges and needn't reach their ends.
All inputs are finite; a program needn't handle non-finite values.
Results may differ from the reference program's by a relative error of at most 0.0004.
Values may be sent and summed in bfloat16 or wider, within the bound.
No kernel may reach another device: no remote copies, remote signals or barrier semaphores. Data moves between devices by JAX's collectives and lax.ppermute only.
A program may use at most 384 MiB of HBM per device.

```python
import math
import jax
import jax.numpy as jnp
from jax import lax

D = 4096
FF = 14336
RANK = 16
EXP = 2
PROJ = 2


def with_spikes(result, key, source, target, blocks, factor):
    def block_of(axis_at):
        return (jnp.arange(result.shape[axis_at]) // (result.shape[axis_at] // blocks)).reshape((-1,) + (1,) * (result.ndim - 1 - axis_at))

    first = jax.random.permutation(key, blocks)[block_of(target)]
    second = (block_of(target) + blocks // 2) % blocks
    return jnp.where((block_of(source) == first) | (block_of(source) == second), factor * result, result)


def block_scale(key, shape, pieces, low, high):
    def one(dim, parts):
        heights = jax.random.uniform(jax.random.fold_in(jax.random.fold_in(key, 6), dim), (parts,), jnp.float32, low / len(pieces), high / len(pieces))
        return jnp.repeat(jnp.exp(heights), shape[dim] // parts).reshape((-1,) + (1,) * (len(shape) - dim - 1))

    level = one(*pieces[0])
    for cut in pieces[1:]:
        level = level * one(*cut)
    return level


def noise(rng, extent, scale, bound, cuts=(), dtype=jnp.bfloat16):
    entries = scale * jax.random.normal(rng, extent, jnp.float32)
    if cuts:
        entries = entries * block_scale(rng, extent, cuts, -0.22, 0.18)
    return jnp.clip(entries, -bound, bound).astype(dtype)


def bell_draw_with(stream_key, extent, deviation, most, pieces, heavy, kind=jnp.bfloat16):
    drawn = deviation * jax.random.normal(stream_key, extent, jnp.float32)
    if pieces:
        drawn = drawn * block_scale(stream_key, extent, pieces, -0.22, 0.18)
    return jnp.clip(with_spikes(drawn, jax.random.fold_in(stream_key, 3), *heavy), -most, most).astype(kind)


def setup_inputs(seed: int = 0) -> dict:
    key_of = jax.random.split(jax.random.key(seed), 5)
    return {
        "base_weight": bell_draw_with(key_of[0], (EXP, PROJ, D, FF), D ** -0.5, 0.125, ((2, 8), (3, 4)), (2, 3, 8, 2.0)),
        "adapter_left": noise(key_of[1], (EXP, PROJ, D, RANK), 0.01, 0.059814453, ((2, 8),)),
        "adapter_right": noise(key_of[2], (EXP, PROJ, RANK, FF), RANK ** -0.5, 1.5, ((3, 4),)),
        "magnitude": jnp.clip(jnp.exp(math.log(256.0) - 2.7725887 * jax.random.uniform(key_of[3], (EXP, PROJ, FF), jnp.float32) ** block_scale(key_of[3], (EXP, PROJ, FF), ((2, 4),), -0.2, 0.2)), 16.0, 256.0).astype(jnp.bfloat16),
    }


def merge_one(operands):
    weight, left_factor, right_factor, column_scale = operands
    merged = weight.astype(jnp.float32) + jnp.dot(left_factor, right_factor, preferred_element_type=jnp.float32)
    squares = lax.optimization_barrier(jnp.sum(merged * merged, axis=0))
    scaling = column_scale.astype(jnp.float32) / jnp.sqrt(squares + 1e-06)
    return (merged * scaling[None, :]).astype(jnp.bfloat16).T

def reference(base_weight, adapter_left, adapter_right, magnitude):
    stacked = lax.map(merge_one, (base_weight.reshape(EXP * PROJ, D, FF), adapter_left.reshape(EXP * PROJ, D, RANK), adapter_right.reshape(EXP * PROJ, RANK, FF), magnitude.reshape(EXP * PROJ, FF)))
    return stacked.reshape(EXP, PROJ, FF, D)
```

```python
import functools

import jax
import jax.numpy as jnp
from jax import lax
from jax.experimental import pallas as pl
from jax.experimental.pallas import tpu as pltpu
from jax.sharding import PartitionSpec as P


AXES = ("tensor", "dp")
LANES, SUBLANES = 128, 16


def regroup(weight_slab):
    experts, projections, row_count, col_count = weight_slab.shape
    tensor_count = lax.axis_size("tensor")
    replica_count = lax.axis_size("dp")
    serve_cols = col_count * replica_count // tensor_count
    quartered = lax.all_to_all(weight_slab, "dp", split_axis=2, concat_axis=3, tiled=True)
    grouped = lax.all_to_all(quartered, "tensor", split_axis=3, concat_axis=2, tiled=True)
    collected = lax.all_gather(grouped, "dp", axis=2, tiled=True)
    pieces_view = collected.reshape(
        experts, projections, replica_count, tensor_count, row_count // replica_count, serve_cols
    )
    return pieces_view.transpose(0, 1, 5, 3, 2, 4).reshape(
        experts, projections, serve_cols, tensor_count * row_count
    )


def plain(base_weight, adapter_left, adapter_right, magnitude):
    tensor_count = lax.axis_size("tensor")
    replica_count = lax.axis_size("dp")
    col_count = base_weight.shape[3]
    serve_cols = col_count * replica_count // tensor_count
    arrived = regroup(base_weight)
    left_full = lax.all_gather(adapter_left, "tensor", axis=2, tiled=True)
    right_all, magnitude_all = (
        lax.all_gather(adapter_right, "dp", axis=3, tiled=True),
        lax.all_gather(magnitude, "dp", axis=2, tiled=True),
    )
    col_start = lax.axis_index("tensor") * serve_cols
    right_cols = lax.dynamic_slice_in_dim(right_all, col_start, serve_cols, 3)
    magnitude_cols = lax.dynamic_slice_in_dim(magnitude_all, col_start, serve_cols, 2)
    merged = arrived.astype(jnp.float32) + jnp.einsum(
        "xyrf,xyir->xyfi", right_cols, left_full, preferred_element_type=jnp.float32
    )
    squares = jnp.sum(merged * merged, axis=3)
    scaling = magnitude_cols.astype(jnp.float32) / jnp.sqrt(squares + 1e-06)
    return (merged * scaling[:, :, :, None]).astype(jnp.bfloat16)


def merged_block(base_ref, left_ref, right_ref):
    low_rank = lax.dot_general(
        left_ref[0], right_ref[0], (((0,), (0,)), ((), ())), preferred_element_type=jnp.float32
    )
    return base_ref[0].astype(jnp.float32) + low_rank


def squares_kernel(base_ref, left_ref, right_ref, out_ref):
    merged = merged_block(base_ref, left_ref, right_ref)
    out_ref[0] = jnp.sum(merged * merged, axis=0, keepdims=True)


def partial_squares(base, left, right):
    units, rows, cols = base.shape
    rank = left.shape[1]
    return pl.pallas_call(
        squares_kernel,
        grid=(units,),
        in_specs=[
            pl.BlockSpec((1, rows, cols), lambda u: (u, 0, 0)),
            pl.BlockSpec((1, rank, rows), lambda u: (u, 0, 0)),
            pl.BlockSpec((1, rank, cols), lambda u: (u, 0, 0)),
        ],
        out_specs=pl.BlockSpec((1, 1, cols), lambda u: (u, 0, 0)),
        out_shape=jax.ShapeDtypeStruct((units, 1, cols), jnp.float32),
        cost_estimate=pl.CostEstimate(
            flops=40 * base.size, bytes_accessed=2 * base.size, transcendentals=0
        ),
        name="partial_squares",
    )(base, left, right)


def scaled_kernel(split, rounds, where_ref, *refs):
    left_ref = refs[0]
    ins, outs = refs[1 : 1 + 3 * rounds], refs[1 + 3 * rounds :]
    for a in range(rounds):
        base_ref, right_ref, scale_ref = ins[3 * a : 3 * a + 3]
        whole_ref, top_ref = outs[2 * a : 2 * a + 2]
        merged = merged_block(base_ref, left_ref, right_ref)
        turned = (merged * scale_ref[0]).astype(jnp.bfloat16).T
        whole_ref[...] = turned
        top_ref[...] = turned[:split]


def scaled_unit(unit, base, left, right, scale, where, rounds, split):
    _, rows, cols = base.shape
    rank = left.shape[1]
    serve = cols // rounds
    width = 2 * LANES if rows % (2 * LANES) == 0 else LANES
    in_specs = [pl.BlockSpec((1, rank, width), lambda b, w: (unit, 0, b))]
    operands = [left]
    out_specs, out_shape = [], []
    for a in range(rounds):
        def part(w, a=a):
            return (w[0] + a) % rounds

        in_specs += [
            pl.BlockSpec((1, width, serve), lambda b, w, part=part: (unit, b, part(w))),
            pl.BlockSpec((1, rank, serve), lambda b, w, part=part: (unit, 0, part(w))),
            pl.BlockSpec((1, 1, serve), lambda b, w, part=part: (unit, 0, part(w))),
        ]
        operands += [base, right, scale]
        for count in (serve, split):
            out_specs.append(pl.BlockSpec((count, width), lambda b, w: (0, b)))
            out_shape.append(jax.ShapeDtypeStruct((count, rows), jnp.bfloat16))
    flat = pl.pallas_call(
        functools.partial(scaled_kernel, split, rounds),
        grid_spec=pltpu.PrefetchScalarGridSpec(
            num_scalar_prefetch=1, grid=(rows // width,), in_specs=in_specs, out_specs=out_specs
        ),
        out_shape=out_shape,
        cost_estimate=pl.CostEstimate(
            flops=40 * rows * cols, bytes_accessed=6 * rows * cols, transcendentals=0
        ),
        name="scaled_unit",
    )(where, *operands)
    return [flat[2 * a : 2 * a + 2] for a in range(rounds)]


def cut_kernel(split, rounds, where_ref, *refs):
    bases, home_ref, lows = refs[:rounds], refs[rounds], refs[rounds + 1 :]
    for a in range(rounds):
        turned = bases[a][0].T
        lows[a][...] = turned[split:]
        if a == 0:
            home_ref[...] = turned


def cut(unit, base, where, rounds, split):
    _, rows, cols = base.shape
    serve = cols // rounds
    width = 2 * LANES if rows % (2 * LANES) == 0 else LANES
    counts = [serve] + [serve - split] * rounds
    home, *lows = pl.pallas_call(
        functools.partial(cut_kernel, split, rounds),
        grid_spec=pltpu.PrefetchScalarGridSpec(
            num_scalar_prefetch=1,
            grid=(rows // width,),
            in_specs=[
                pl.BlockSpec((1, width, serve), lambda b, w, a=a: (unit, b, (w[0] + a) % rounds))
                for a in range(rounds)
            ],
            out_specs=[pl.BlockSpec((count, width), lambda b, w: (0, b)) for count in counts],
        ),
        out_shape=[jax.ShapeDtypeStruct((count, rows), jnp.bfloat16) for count in counts],
        cost_estimate=pl.CostEstimate(
            flops=20 * rows * cols, bytes_accessed=4 * rows * cols, transcendentals=0
        ),
        name="cut",
    )(where, *[base] * rounds)
    return home, lows


def over_kernel(first_row, where_ref, raw_ref, left_ref, right_ref, scale_ref, out_ref):
    low_rank = lax.dot_general(
        right_ref[0], left_ref[0], (((0,), (0,)), ((), ())), preferred_element_type=jnp.float32
    )[first_row:]
    spread = jnp.broadcast_to(scale_ref[0], (LANES, scale_ref.shape[2])).T[first_row:]
    merged = raw_ref[...].astype(jnp.float32) + low_rank
    for at in range(0, merged.shape[1], LANES):
        part = merged[:, at : at + LANES] * spread
        out_ref[:, at : at + LANES] = part.astype(jnp.bfloat16)


def scaled_over(unit, a, raw, left, right, scale, where, rounds, first_row):
    count, rows = raw.shape
    rank, cols = right.shape[1:]
    serve = cols // rounds
    width = 2 * LANES if rows % (2 * LANES) == 0 else LANES

    def part(w):
        return (w[0] + a) % rounds

    return pl.pallas_call(
        functools.partial(over_kernel, first_row),
        grid_spec=pltpu.PrefetchScalarGridSpec(
            num_scalar_prefetch=1,
            grid=(rows // width,),
            in_specs=[
                pl.BlockSpec((count, width), lambda b, w: (0, b)),
                pl.BlockSpec((1, rank, width), lambda b, w: (unit, 0, b)),
                pl.BlockSpec((1, rank, serve), lambda b, w: (unit, 0, part(w))),
                pl.BlockSpec((1, 1, serve), lambda b, w: (unit, 0, part(w))),
            ],
            out_specs=pl.BlockSpec((count, width), lambda b, w: (0, b)),
        ),
        out_shape=jax.ShapeDtypeStruct((count, rows), jnp.bfloat16),
        cost_estimate=pl.CostEstimate(
            flops=40 * count * rows, bytes_accessed=4 * count * rows, transcendentals=0
        ),
        name="scaled_over",
    )(where, raw, left, right, scale)


NEAR, FAR, ANY, SAME, OTHER = 1, 0, None, 1, 0


class Piece:
    def __init__(self, holders, a, is_far, first_row):
        self.holders = holders
        count, self.rows = holders[0][0].shape
        self.mark = ([h[1:] for h in holders], a, is_far, first_row, count)


def target(out_ref, unit, rounds, rows, where_ref, core, mark):
    _, a, is_far, first_row, count = mark
    half = 1 - where_ref[1] if is_far else where_ref[1]
    lane = ((2 * half + core) * rounds + (where_ref[0] + rounds - a) % rounds) * rows
    return out_ref.at[unit, pl.ds(first_row, count), pl.ds(pl.multiple_of(lane, LANES), rows)]


def collect_kernel(unit, rounds, rows, marks, has_out, where_ref, *refs):
    inputs = sum(len(mark[0]) for mark in marks)
    ins, rest = list(refs[:inputs]), refs[inputs + has_out :]
    mine_ref, out_ref = rest[:2]
    buffers, in_sems, out_sems = rest[2:-2], rest[-2], rest[-1]
    is_near, core, same = where_ref[2], where_ref[3], where_ref[4]
    sources = []
    for n, mark in enumerate(marks):
        for who, which in mark[0]:
            source = ins.pop(0)
            here = is_near == who
            if which is not ANY:
                here = here & (same == which)

            @pl.when(here)
            def _(source=source, n=n):
                pltpu.make_async_copy(source, buffers[n], in_sems.at[n]).start()

        sources.append(source)
    sent, row = [], 0
    for n, mark in enumerate(marks):
        to_mine = mine_ref.at[pl.ds(row, mark[-1])]
        to_out = target(out_ref, unit, rounds, rows, where_ref, core, mark)
        pltpu.make_async_copy(sources[n], buffers[n], in_sems.at[n]).wait()
        for m, to in enumerate((to_mine, to_out)):
            sent.append(pltpu.make_async_copy(buffers[n], to, out_sems.at[2 * n + m]))
            sent[-1].start()
        row += mark[-1]
    for one in sent:
        one.wait()


def collect(unit, whole, rounds, where, pieces, out):
    rows = pieces[0].rows
    arrays = [h[0] for piece in pieces for h in piece.holders]
    marks = [piece.mark for piece in pieces]
    operands = [where, *arrays] + ([] if out is None else [out])
    height = sum(mark[-1] for mark in marks)
    return pl.pallas_call(
        functools.partial(collect_kernel, unit, rounds, rows, marks, int(out is not None)),
        in_specs=[pl.BlockSpec(memory_space=pltpu.SMEM)]
        + [pl.BlockSpec(memory_space=pl.ANY)] * (len(operands) - 1),
        out_specs=[pl.BlockSpec(memory_space=pl.ANY)] * 2,
        out_shape=[
            jax.ShapeDtypeStruct((height, rows), jnp.bfloat16),
            jax.ShapeDtypeStruct(whole, jnp.bfloat16),
        ],
        input_output_aliases={} if out is None else {len(operands) - 1: 1},
        scratch_shapes=[pltpu.VMEM((mark[-1], rows), jnp.bfloat16) for mark in marks]
        + [pltpu.SemaphoreType.DMA((len(marks),)), pltpu.SemaphoreType.DMA((2 * len(marks),))],
        cost_estimate=pl.CostEstimate(
            flops=20 * height * rows, bytes_accessed=6 * height * rows, transcendentals=0
        ),
        name="collect",
    )(*operands)


def place_kernel(unit, rounds, rows, marks, where_ref, other_ref, out_in_ref, out_ref, *refs):
    buffers, in_sems, out_sems = refs[:-2], refs[-2], refs[-1]
    coming, row = [], 0
    for n, mark in enumerate(marks):
        part = other_ref.at[pl.ds(row, mark[-1])]
        coming.append(pltpu.make_async_copy(part, buffers[n], in_sems.at[n]))
        coming[-1].start()
        row += mark[-1]
    sent = []
    for n, mark in enumerate(marks):
        to_out = target(out_ref, unit, rounds, rows, where_ref, 1 - where_ref[3], mark)
        coming[n].wait()
        sent.append(pltpu.make_async_copy(buffers[n], to_out, out_sems.at[n]))
        sent[-1].start()
    for one in sent:
        one.wait()


def place(unit, rounds, where, pieces, other, out):
    rows = pieces[0].rows
    marks = [piece.mark for piece in pieces]
    return pl.pallas_call(
        functools.partial(place_kernel, unit, rounds, rows, marks),
        in_specs=[pl.BlockSpec(memory_space=pltpu.SMEM)]
        + [pl.BlockSpec(memory_space=pl.ANY)] * 2,
        out_specs=pl.BlockSpec(memory_space=pl.ANY),
        out_shape=jax.ShapeDtypeStruct(out.shape, out.dtype),
        input_output_aliases={2: 0},
        scratch_shapes=[pltpu.VMEM((mark[-1], rows), jnp.bfloat16) for mark in marks]
        + [pltpu.SemaphoreType.DMA((len(marks),))] * 2,
        cost_estimate=pl.CostEstimate(
            flops=20 * other.size, bytes_accessed=4 * other.size, transcendentals=0
        ),
        name="place",
    )(where, other, out)


class Routes:
    def __init__(self, rounds):
        self.rounds = rounds
        self.devices = [
            (z, y, x, c) for z in range(4) for y in range(rounds) for x in range(2) for c in range(2)
        ]

    def pairs(self, keep, to):
        def number(z, y, x, c):
            return (z * self.rounds + y) * 4 + 2 * x + c

        made = [(number(*s), number(*to(*s))) for s in self.devices if keep(*s)]
        return [(source, target) for source, target in made if source != target]

    def near(self, z, y, x, c):
        return z // 2 == x

    def near_same(self, z, y, x, c):
        return z // 2 == x and z % 2 == c

    def near_other(self, z, y, x, c):
        return z // 2 == x and z % 2 != c

    def far(self, z, y, x, c):
        return z // 2 != x

    def everyone(self, z, y, x, c):
        return True

    def over_x(self, keep):
        return self.pairs(keep, lambda z, y, x, c: (z, y, 1 - x, c))

    def over_core(self):
        return self.pairs(self.everyone, lambda z, y, x, c: (z, y, x, 1 - c))

    def serve(self, keep, a, crossed):
        def to(z, y, x, c):
            owner = 1 - x if crossed else x
            return (2 * owner + c, (y + a) % self.rounds, x, z % 2)

        return self.pairs(keep, to)

    def fold(self, step):
        def to(z, y, x, c):
            t = (z * self.rounds + y) ^ step
            return (t // self.rounds, t % self.rounds, x, c)

        return self.pairs(self.everyone, to)


def move(value, pairs):
    return lax.ppermute(value, AXES, pairs)


def routed(base_weight, adapter_left, adapter_right, magnitude):
    tensor_count = lax.axis_size("tensor")
    rounds = tensor_count // lax.axis_size("dp")
    routes = Routes(rounds)
    experts, projections, rows, cols = base_weight.shape
    units = experts * projections
    rank = adapter_left.shape[3]
    serve = cols // rounds
    base = base_weight.reshape(units, rows, cols)
    left = jnp.swapaxes(adapter_left.reshape(units, rows, rank), 1, 2)
    right = adapter_right.reshape(units, rank, cols)
    spot, replica = lax.axis_index("tensor"), lax.axis_index("dp")
    z, y, x, c = spot // rounds, spot % rounds, replica // 2, replica % 2
    is_near = (z // 2 == x).astype(jnp.int32)
    where = jnp.stack([y, z // 2, is_near, c, z % 2 == c]).astype(jnp.int32)
    split = top_rows(serve)

    turns = range(rounds)

    over_x = routes.over_x(routes.everyone)
    raws = []
    for unit in range(units):
        raws.append(cut(unit, base, where, rounds, split))
    right_over = move(right, over_x)

    squares = partial_squares(base, left, right)
    step = 1
    while step < tensor_count:
        squares = squares + move(squares, routes.fold(step))
        step *= 2
    scale = magnitude.reshape(units, 1, cols).astype(jnp.float32) / jnp.sqrt(squares + 1e-06)
    scale_over = move(scale, over_x)

    def over(unit, a, raw, first_row):
        return scaled_over(
            unit, a, raw, left, right_over, scale_over, where, rounds, first_row
        )

    def moved(values, pairs_of):
        made = []
        for a in turns:
            made.append(move(values[a], pairs_of(a)))
        return made

    def to_far(a):
        return routes.over_x(routes.near)

    def to_near(a):
        return routes.over_x(routes.far)

    landed = []
    for unit in range(units):
        parts = scaled_unit(unit, base, left, right, scale, where, rounds, split)
        raw_s = moved(raws[unit][1], to_near)
        low_s = [over(unit, a, raw_s[a], split) for a in turns]
        near_l = moved([p[0] for p in parts], lambda a: routes.serve(routes.near, a, False))
        top_l = moved([p[1] for p in parts], lambda a: routes.serve(routes.far, a, False))
        low_l = moved(low_s, lambda a: routes.serve(routes.near, a, True))
        home_x = move(raws[unit][0], routes.over_x(routes.near_same))
        home_x = over(unit, 0, home_x, 0)
        near_x = moved(near_l, lambda a: routes.over_x(routes.near if a else routes.near_other))
        top_x = moved(top_l, to_far)
        low_x = moved(low_l, to_near)
        near = [[(near_l[a], NEAR, ANY), (near_x[a], FAR, ANY)] for a in turns]
        near[0] = [
            (parts[0][0], NEAR, SAME),
            (near_l[0], NEAR, OTHER),
            (home_x, FAR, SAME),
            (near_x[0], FAR, OTHER),
        ]
        pieces = {}
        for a in turns:
            pieces["near", a] = Piece(near[a], a, False, 0)
            top = [(top_l[a], NEAR, ANY), (top_x[a], FAR, ANY)]
            pieces["top", a] = Piece(top, a, True, 0)
            low = [(low_x[a], NEAR, ANY), (low_l[a], FAR, ANY)]
            pieces["low", a] = Piece(low, a, True, split)
        landed.append(pieces)
    out, others = None, {}
    whole = (units, serve, tensor_count * rows)
    for kind, name, unit, keys in finish_order(units, rounds):
        pieces = [landed[unit][key] for key in keys]
        if kind == "collect":
            mine, out = collect(unit, whole, rounds, where, pieces, out)
        else:
            out = place(unit, rounds, where, pieces, others[unit, name], out)
        if kind == "collect":
            others[unit, name] = move(mine, routes.over_core())
    return out.reshape(experts, projections, serve, tensor_count * rows)


def finish_order(units, rounds):
    turns = range(rounds)
    order = []
    for unit in range(units):
        if unit < units - 1:
            parts = [("", [(kind, a) for kind in ("near", "top", "low") for a in turns])]
        else:
            parts = [("A", [("near", a) for a in turns])]
            parts += [("BCDEFGHIJ"[a], [("top", a), ("low", a)]) for a in turns]
        for name, keys in parts:
            order.append(("collect", name, unit, keys))
            before = [o for o in order if o[0] == "collect"][-2:-1]
            order += [("place", *o[1:]) for o in before]
    return order + [("place", *order[-2][1:])]


def top_rows(serve):
    return max(1, round(serve * 0.4 / SUBLANES)) * SUBLANES


def takes_routes(mesh, rows, cols):
    tensor_count, replicas = mesh.shape["tensor"], mesh.shape["dp"]
    if replicas != 4 or tensor_count % replicas or tensor_count & (tensor_count - 1):
        return False
    serve = cols * 1 // tensor_count
    return (rows // tensor_count) % LANES == 0 and serve % LANES == 0 and serve >= 2 * LANES


def solution(mesh):
    in_specs = (
        P(None, None, "tensor", "dp"),
        P(None, None, "tensor", None),
        P(None, None, None, "dp"),
        P(None, None, "dp"),
    )
    out_specs = P(None, None, "tensor", None)

    def whole(base_weight, adapter_left, adapter_right, magnitude):
        _, _, rows, cols = base_weight.shape
        fits = takes_routes(mesh, rows, cols)
        body = jax.shard_map(
            routed if fits else plain,
            mesh=mesh,
            in_specs=in_specs,
            out_specs=out_specs,
            check_vma=False,
        )
        return body(base_weight, adapter_left, adapter_right, magnitude)

    return whole
```
